16 devices in a mesh: dp: 1, ep: 16 (over x, y, z, core).
Axes of the slice: x: 2, y: 2, z: 2, core: 2. Of those that a mesh axis runs over, the one named last changes fastest.
Arguments:
- x: bfloat16 [1, 16, 256, 2560], P('dp', 'ep')
- expert: int32 [1, 16, 256, 8], P('dp', 'ep')
- slot: int32 [1, 16, 256, 8], P('dp', 'ep')
- gate: float32 [1, 16, 256, 8], P('dp', 'ep')
- w_gate: bfloat16 [80, 2560, 1536], P('ep')
- w_up: bfloat16 [80, 2560, 1536], P('ep')
- w_down: bfloat16 [80, 1536, 2560], P('ep')
- s_gate: bfloat16 [2560, 1536], replicated
- s_up: bfloat16 [2560, 1536], replicated
- s_down: bfloat16 [1536, 2560], replicated
Outputs:
- y: bfloat16 [1, 16, 256, 2560], P('dp', 'ep')
All inputs are finite; a program needn't handle non-finite values.
Results may differ from the reference program's by a relative error of at most 0.009.
Values are sent between devices in bfloat16 or wider.
A program may use at most 2 GiB of HBM per device.

```python
import jax
import jax.numpy as jnp

MEMBERS = 16
TOKENS = 256
D = 2560
FF = 1536
TOP = 8
EXPERTS = 80
SHARED_FF = 1536
SLOTS = 5 * TOKENS * TOP // (4 * EXPERTS)


def setup_inputs(seed: int = 0, part: int = 0) -> dict:
    own, k1, k2, k3, k4, k5, k6 = jax.random.split(jax.random.key(seed), 7)
    kx, ke, kl, kg = jax.random.split(jax.random.fold_in(own, part), 4)
    devices = (1, MEMBERS)
    place = jax.random.permutation(kl, jnp.arange(EXPERTS, dtype=jnp.uint32))
    slow = ((EXPERTS + (9 * place) % EXPERTS) << ((9 * place) // EXPERTS)) // EXPERTS
    wait = (jax.random.bits(ke, (*devices, TOKENS, EXPERTS), jnp.uint32) >> 10) * slow
    expert = jnp.argsort(wait, axis=-1)[..., :TOP].astype(jnp.int32)
    chosen = jax.nn.one_hot(expert, EXPERTS, dtype=jnp.int32)
    in_line = jnp.cumsum(chosen.reshape(*devices, TOKENS * TOP, EXPERTS), axis=2) - 1
    slot = jnp.sum(in_line.reshape(chosen.shape) * chosen, axis=-1)

    def one(key, rows, columns):
        return (jax.random.normal(key, (rows, columns), jnp.float32) * rows**-0.5).astype(jnp.bfloat16)

    def weights(key, rows, columns):
        return jax.lax.map(lambda k: one(k, rows, columns), jax.random.split(key, EXPERTS))

    return {
        "x": jax.random.normal(kx, (*devices, TOKENS, D), jnp.float32).astype(jnp.bfloat16),
        "expert": expert,
        "slot": slot,
        "gate": jax.nn.softmax(jax.random.normal(kg, expert.shape, jnp.float32)),
        "w_gate": weights(k1, D, FF),
        "w_up": weights(k2, D, FF),
        "w_down": weights(k3, FF, D),
        "s_gate": one(k4, D, SHARED_FF),
        "s_up": one(k5, D, SHARED_FF),
        "s_down": one(k6, SHARED_FF, D),
    }


def einsum(form, a, b):
    return jnp.einsum(form, a.astype(jnp.float32), b.astype(jnp.float32))


def for_all(x, s_gate, s_up, s_down):
    h = jax.nn.silu(einsum("...d,df->...f", x, s_gate)) * einsum("...d,df->...f", x, s_up)
    return einsum("...f,fd->...d", h.astype(jnp.bfloat16), s_down)


def reference(x, expert, slot, gate, w_gate, w_up, w_down, s_gate, s_up, s_down):
    to_expert = jax.nn.one_hot(expert, EXPERTS, dtype=jnp.bfloat16)
    to_slot = jax.nn.one_hot(slot, SLOTS, dtype=jnp.bfloat16)
    weighted = to_expert * gate[..., None].astype(jnp.bfloat16)
    dispatch = einsum("abtke,abtkc->abtec", to_expert, to_slot).astype(jnp.bfloat16)
    combine = einsum("abtke,abtkc->abtec", weighted, to_slot).astype(jnp.bfloat16)
    z = einsum("abtec,abtd->aebcd", dispatch, x).astype(jnp.bfloat16)
    h = jax.nn.silu(einsum("aebcd,edf->aebcf", z, w_gate))
    h = (h * einsum("aebcd,edf->aebcf", z, w_up)).astype(jnp.bfloat16)
    out = einsum("aebcf,efd->aebcd", h, w_down).astype(jnp.bfloat16)
    y = einsum("abtec,aebcd->abtd", combine, out)
    return (y + for_all(x, s_gate, s_up, s_down)).astype(jnp.bfloat16)
```

```python
import functools

import jax
import jax.numpy as jnp
from jax import lax
from jax.experimental import pallas as pl
from jax.experimental.pallas import tpu as pltpu
from jax.sharding import PartitionSpec as P

MESH = pl.DeviceIdType.MESH
F32, BF16 = jnp.float32, jnp.bfloat16
ROWS = ((0, 96), (96, 80), (176, 80))
KU, KW = 5, 512
NU, NW = 10, 256
NE, CAP = 5, 32
RING = 5
PRE = 4
HB = 40


def kernel(meta_ref, x_ref, wg_ref, wu_ref, wd_ref, sg_ref, su_ref, sd_ref, y_ref,
           gmeta, onehot, comb, xg, acc, z, wgu, wdn, ys, ob, rc, rb, ra, sc, sb, sa, yst,
           m_send, m_recv, ag_a, ag_b, ag_c, ag_p, ag_s, ag_ps, free,
           gu_sem, dn_sem, o_recv, o_send, o_free, c_recv, b_recv, a_recv, c_send, b_send, a_send, y_sem):
    me = lax.axis_index("ep")
    core = me % 2
    chip = me // 2
    partner = me + 1 - 2 * core
    dx = 4 * (1 - 2 * ((chip // 4) % 2))
    dy = 2 * (1 - 2 * ((chip // 2) % 2))
    dz = 1 - 2 * (chip % 2)

    def delta(t):
        return dx + t * (dy - dx) + ((t * (t - 1)) // 2) * (dz - 2 * dy + dx)

    def order(i, u):
        return delta((i + u) % 3), delta((i + u + 1) % 3), delta((i + u + 2) % 3)

    def peer(d):
        return 2 * (chip + d) + core

    def remote(src, dst, send, recv, dev):
        return pltpu.make_async_remote_copy(
            src_ref=src, dst_ref=dst, send_sem=send, recv_sem=recv, device_id={"ep": dev}, device_id_type=MESH)

    def start_gu(i):
        slot = i % 2

        @pl.when(i < KU)
        def _():
            rows = pl.ds(pl.multiple_of(i * KW, KW), KW)
            pltpu.make_async_copy(sg_ref.at[rows], wgu.at[slot, 0], gu_sem.at[slot, 0]).start()
            pltpu.make_async_copy(su_ref.at[rows], wgu.at[slot, 1], gu_sem.at[slot, 1]).start()

        @pl.when(jnp.logical_and(i >= KU, i < KU + 2 * KU * NE))
        def _():
            m = (i - KU) % (KU * NE)
            rows = pl.ds(pl.multiple_of((m // NE) * KW, KW), KW)
            pltpu.make_async_copy(wg_ref.at[m % NE, rows], wgu.at[slot, 0], gu_sem.at[slot, 0]).start()
            pltpu.make_async_copy(wu_ref.at[m % NE, rows], wgu.at[slot, 1], gu_sem.at[slot, 1]).start()

    def wait_gu(i):
        slot = i % 2
        for j in range(2):
            pltpu.make_async_copy(sg_ref.at[pl.ds(0, KW)], wgu.at[slot, j], gu_sem.at[slot, j]).wait()

    def start_dn(i):
        slot = i % 3

        @pl.when(i < NU)
        def _():
            cols = pl.ds(pl.multiple_of(i * NW, NW), NW)
            pltpu.make_async_copy(sd_ref.at[:, cols], wdn.at[slot], dn_sem.at[slot]).start()

        @pl.when(jnp.logical_and(i >= NU, i < NU + 2 * NU * NE))
        def _():
            m = i - NU
            cols = pl.ds(pl.multiple_of(((m // NE) % NU) * NW, NW), NW)
            pltpu.make_async_copy(wd_ref.at[m % NE, :, cols], wdn.at[slot], dn_sem.at[slot]).start()

    def wait_dn(i):
        slot = i % 3
        pltpu.make_async_copy(sd_ref.at[:, pl.ds(0, NW)], wdn.at[slot], dn_sem.at[slot]).wait()

    def blk(k, s):
        return k * 8 + s

    def own(q):
        k = q % KU
        cols = pl.ds(pl.multiple_of(k * KW, KW), KW)

        @pl.when(q >= KU)
        def _():
            pl.semaphore_wait(free.at[k], 4)

        for stage, sem in enumerate((ag_a, ag_b, ag_c)):
            for i, (r0, rn) in enumerate(ROWS):
                d = order(i, k)[stage]
                remote(x_ref.at[pl.ds(r0, rn), cols], xg.at[blk(k, chip), pl.ds(r0, rn)],
                       ag_s.at[k], sem.at[k], peer(d)).start()
        remote(x_ref.at[:, cols], xg.at[blk(k, chip)], ag_ps.at[k], ag_p.at[k], partner).start()
        xg[blk(k, chip)] = x_ref[:, cols]

    def arrived(sem, k, n):
        remote(xg.at[pl.ds(0, n)], xg.at[pl.ds(0, n)], ag_s.at[k], sem.at[k], partner).wait_recv()

    def forward(b, r0, rn, k, sem, dev):
        part = xg.at[b, pl.ds(r0, rn)]
        remote(part, part, ag_s.at[k], sem.at[k], dev).start()

    def forward_p(b, r0, rn, k):
        part = xg.at[b, pl.ds(r0, rn)]
        remote(part, part, ag_ps.at[k], ag_p.at[k], partner).start()

    def event_a(k):
        arrived(ag_a, k, 1)
        for i, (r0, rn) in enumerate(ROWS):
            a, b, c = order(i, k)
            forward(blk(k, chip + a), r0, rn, k, ag_b, peer(b))
        for i, (r0, rn) in enumerate(ROWS):
            a, b, c = order(i, k)
            forward(blk(k, chip + a), r0, rn, k, ag_c, peer(c))
        for i, (r0, rn) in enumerate(ROWS):
            a, b, c = order(i, k)
            forward_p(blk(k, chip + a), r0, rn, k)

    def event_b(k):
        arrived(ag_b, k, 2)
        for i, (r0, rn) in enumerate(ROWS):
            a, b, c = order(i, k)
            forward(blk(k, chip + b), r0, rn, k, ag_c, peer(c))
            forward(blk(k, chip + b + a), r0, rn, k, ag_c, peer(c))
        for i, (r0, rn) in enumerate(ROWS):
            a, b, c = order(i, k)
            forward_p(blk(k, chip + b), r0, rn, k)
            forward_p(blk(k, chip + b + a), r0, rn, k)

    def event_c(k):
        arrived(ag_c, k, 4)
        for i, (r0, rn) in enumerate(ROWS):
            a, b, c = order(i, k)
            for d in (c, c + a, c + b, c + b + a):
                forward_p(blk(k, chip + d), r0, rn, k)

    def sent(k):
        remote(xg.at[pl.ds(0, 7)], xg.at[pl.ds(0, 7)], ag_s.at[k], ag_a.at[k], partner).wait_send()
        remote(xg.at[pl.ds(0, 8)], xg.at[pl.ds(0, 8)], ag_ps.at[k], ag_p.at[k], partner).wait_send()

    def act(n, store):
        def body(t, _):
            e, r = t // 8, t % 8
            rows = pl.ds(pl.multiple_of(r * 32, 32), 32)
            for q in range(3):
                cols = slice(q * KW, (q + 1) * KW)
                g = acc[e, 0, rows, cols]
                u = acc[e, 1, rows, cols]
                acc[e, 0, rows, cols] = jnp.zeros((32, KW), F32)
                acc[e, 1, rows, cols] = jnp.zeros((32, KW), F32)
                store(e, q, rows, (g * (1.0 / (1.0 + jnp.exp(-g))) * u).astype(BF16))
            return 0

        lax.fori_loop(0, n * 8, body, 0)

    def gate_up(i, lhs, e):
        wait_gu(i)
        slot = i % 2
        for j in range(2):
            acc[e, j] += jnp.dot(lhs, wgu[slot, j], preferred_element_type=F32)
        start_gu(i + 2)

    for i in range(2):
        start_gu(jnp.int32(i))
    for i in range(3):
        start_dn(jnp.int32(i))
    barrier = pltpu.get_barrier_semaphore()

    def greet(i, _):
        pl.semaphore_signal(barrier, inc=1, device_id={"ep": (me + i) % 16}, device_id_type=MESH)
        return 0

    lax.fori_loop(1, 16, greet, 0)
    pl.semaphore_wait(barrier, 15)

    @pl.when(core == 0)
    def _():
        own(jnp.int32(0))

    def tell(i, _):
        remote(meta_ref, gmeta.at[me], m_send, m_recv, (me + i) % 16).start()
        return 0

    lax.fori_loop(1, 16, tell, 0)
    gmeta[me] = meta_ref[...]

    @pl.when(core == 0)
    def _():
        own(jnp.int32(1))

    def clear(t, _):
        e, r = t // 8, t % 8
        rows = pl.ds(pl.multiple_of(r * 32, 32), 32)
        for j in range(2):
            acc[e, j, rows] = jnp.zeros((32, 1536), F32)
        return 0

    lax.fori_loop(0, NE * 8, clear, 0)

    def shared(i, _):
        @pl.when(jnp.logical_and(core == 0, i == 1))
        def _():
            event_a(jnp.int32(0))

        @pl.when(jnp.logical_and(core == 0, i == 4))
        def _():
            event_b(jnp.int32(0))

        gate_up(i, x_ref[:, pl.ds(pl.multiple_of(i * KW, KW), KW)], 0)
        return 0

    lax.fori_loop(0, KU, shared, 0)

    def store_shared(e, q, rows, v):
        z[q, rows] = v

    act(1, store_shared)

    def shared_down(i, _):
        wait_dn(i)
        slot = i % 3
        ys[i] = sum(jnp.dot(z[q], wdn[slot, q * KW:(q + 1) * KW], preferred_element_type=F32) for q in range(3))
        start_dn(i + 3)
        return 0

    lax.fori_loop(0, NU, shared_down, 0)

    remote(gmeta.at[pl.ds(0, 15)], gmeta.at[pl.ds(0, 15)], m_send, m_recv, partner).wait()

    def build_comb(s, _):
        m = gmeta[2 * s + core]
        row = lax.broadcasted_iota(jnp.int32, (384, 256), 0)
        mine = (me * (NE * CAP)).astype(jnp.int32)
        theirs = (partner * (NE * CAP)).astype(jnp.int32)
        target = jnp.where(row < 160, row + mine, jnp.where(row < 320, row - 160 + theirs, -7)).astype(F32)
        t = jnp.zeros((384, 256), F32)
        for j in range(8):
            t = t + jnp.where(target == m[j:j + 1], m[8 + j:9 + j], 0.0)
        comb[s] = t.T.astype(BF16)
        return 0

    lax.fori_loop(0, 8, build_comb, 0)

    def gather_step(g):
        ph, k = g // KU, g % KU
        nxt = g + 1

        @pl.when(core == ph)
        def _():
            event_c(k)

        @pl.when(core != ph)
        def _():
            arrived(ag_p, k, 8)

        @pl.when(jnp.logical_and(nxt < 2 * KU, core == nxt // KU))
        def _():
            event_a(nxt % KU)

        @pl.when(k == 0)
        def _():
            def build(s, _):
                m = gmeta[2 * s + ph]
                target = (lax.broadcasted_iota(jnp.int32, (160, 256), 0) + me * (NE * CAP)).astype(F32)
                t = jnp.zeros((160, 256), F32)
                for j in range(8):
                    t = jnp.where(target == m[j:j + 1], 1.0, t)
                onehot[s] = t.astype(BF16)
                return 0

            lax.fori_loop(0, 8, build, 0)

        for s in range(8):
            zs = jnp.dot(onehot[s], xg[blk(k, s)], preferred_element_type=F32).astype(BF16)
            for e in range(NE):
                z[e, s * CAP:(s + 1) * CAP] = zs[e * CAP:(e + 1) * CAP]

        def expert(e, _):
            @pl.when(e == 2)
            def _():
                @pl.when(jnp.logical_and(nxt < 2 * KU, core == nxt // KU))
                def _():
                    event_b(nxt % KU)

                @pl.when(jnp.logical_and(g + 2 < 2 * KU, core == (g + 2) // KU))
                def _():
                    own(g + 2)

            gate_up(KU + g * NE + e, z[e], e)
            return 0

        lax.fori_loop(0, NE, expert, 0)

        @pl.when(jnp.logical_and(ph == 0, core == 0))
        def _():
            sent(k)
            pl.semaphore_signal(free.at[k], inc=1, device_id={"ep": partner}, device_id_type=MESH)

        @pl.when(jnp.logical_and(ph == 0, core == 1))
        def _():
            for d in (dx, dy, dz):
                pl.semaphore_signal(free.at[k], inc=1, device_id={"ep": peer(d)}, device_id_type=MESH)

        @pl.when(k == KU - 1)
        def _():
            @pl.when(jnp.logical_and(ph == 1, core == 1))
            def _():
                for kk in range(KU):
                    sent(kk)

            def store(e, q, rows, v):
                xg[HB * (1 - ph) + e * 3 + q, rows] = v

            act(NE, store)

    def term(slot, d, r0, rn):
        return jnp.dot(comb[d, r0:r0 + rn, :320], ob[slot, d], preferred_element_type=F32)

    def sum_step(r):
        def main(v):
            return jnp.logical_and(jnp.logical_and(v >= 0, v < 2 * NU), core == v // NU)

        v4 = r - 5

        @pl.when(main(v4))
        def _():
            u, slot, p = v4 % NU, v4 % RING, v4 % 2
            remote(ra.at[u], ra.at[u], a_send.at[0], a_recv.at[u], partner).wait_recv()
            val = term(slot, chip, 0, 256) + rc[u, 0].astype(F32) + rb[u, 0].astype(F32) + ra[u].astype(F32) + ys[u]

            @pl.when(u >= 2)
            def _():
                pltpu.make_async_copy(yst.at[p], y_ref.at[:, pl.ds(0, NW)], y_sem.at[p]).wait()

            yst[p] = val.astype(BF16)
            cols = pl.ds(pl.multiple_of(u * NW, NW), NW)
            pltpu.make_async_copy(yst.at[p], y_ref.at[:, cols], y_sem.at[p]).start()

            @pl.when(u < NU - RING)
            def _():
                pl.semaphore_signal(o_free, inc=1, device_id={"ep": partner}, device_id_type=MESH)

        v3 = r - 4

        @pl.when(main(v3))
        def _():
            u, slot, p = v3 % NU, v3 % RING, v3 % 2
            remote(rb.at[u], rb.at[u], b_send.at[0], b_recv.at[u], partner).wait_recv()

            @pl.when(u >= 2)
            def _():
                remote(sa.at[p], sa.at[p], a_send.at[p], a_recv.at[0], partner).wait_send()

            for i, (r0, rn) in enumerate(ROWS):
                a, b, c = order(i, u)
                rows = slice(r0, r0 + rn)
                val = term(slot, chip + a, r0, rn) + rc[u, 1, rows].astype(F32) + rb[u, 1, rows].astype(F32)
                sa[p, rows] = val.astype(BF16)
            for i, (r0, rn) in enumerate(ROWS):
                a, b, c = order(i, u)
                remote(sa.at[p, pl.ds(r0, rn)], ra.at[u, pl.ds(r0, rn)], a_send.at[p], a_recv.at[u], peer(a)).start()

        v2 = r - 3

        @pl.when(main(v2))
        def _():
            u, slot, p = v2 % NU, v2 % RING, v2 % 2
            remote(rc.at[u], rc.at[u], c_send.at[0], c_recv.at[u], partner).wait_recv()

            @pl.when(u >= 2)
            def _():
                remote(sb.at[p], sb.at[p], b_send.at[p], b_recv.at[0], partner).wait_send()

            for i, (r0, rn) in enumerate(ROWS):
                a, b, c = order(i, u)
                rows = slice(r0, r0 + rn)
                for h in range(2):
                    val = term(slot, chip + b + h * a, r0, rn) + rc[u, 2 + h, rows].astype(F32)
                    sb[p, h, rows] = val.astype(BF16)
            for i, (r0, rn) in enumerate(ROWS):
                a, b, c = order(i, u)
                remote(sb.at[p, :, pl.ds(r0, rn)], rb.at[u, :, pl.ds(r0, rn)], b_send.at[p], b_recv.at[u],
                       peer(b)).start()

        @pl.when(r < 2 * NU)
        def _():
            ph, slot = r // NU, r % RING

            for e in range(NE):
                i = NU + r * NE + e
                wait_dn(i)
                o = sum(jnp.dot(xg[HB * (1 - ph) + e * 3 + q], wdn[i % 3, q * KW:(q + 1) * KW],
                                preferred_element_type=F32) for q in range(3)).astype(BF16)
                for s in range(8):
                    ob[slot, s, e * CAP:(e + 1) * CAP] = o[s * CAP:(s + 1) * CAP]
                start_dn(i + 3)

            @pl.when(core != ph)
            def _():
                @pl.when(r % NU >= RING)
                def _():
                    pl.semaphore_wait(o_free, 1)

                remote(ob.at[slot, :, pl.ds(0, 160)], ob.at[slot, :, pl.ds(160, 160)], o_send.at[slot],
                       o_recv.at[slot], partner).start()

        v1 = r - 1

        @pl.when(main(v1))
        def _():
            u, slot, p = v1 % NU, v1 % RING, v1 % 2
            part = ob.at[slot, :, pl.ds(160, 160)]
            remote(part, part, o_send.at[slot], o_recv.at[slot], partner).wait_recv()

            @pl.when(u >= 2)
            def _():
                remote(sc.at[p], sc.at[p], c_send.at[p], c_recv.at[0], partner).wait_send()

            for i, (r0, rn) in enumerate(ROWS):
                a, b, c = order(i, u)
                rows = slice(r0, r0 + rn)
                for h in range(4):
                    val = term(slot, chip + c + (h // 2) * b + (h % 2) * a, r0, rn)
                    sc[p, h, rows] = val.astype(BF16)
            for i, (r0, rn) in enumerate(ROWS):
                a, b, c = order(i, u)
                remote(sc.at[p, :, pl.ds(r0, rn)], rc.at[u, :, pl.ds(r0, rn)], c_send.at[p], c_recv.at[u],
                       peer(c)).start()

    def drained(r):
        v = r - RING

        @pl.when(jnp.logical_and(v >= 0, core != v // NU))
        def _():
            slot = v % RING
            part = ob.at[slot, :, pl.ds(0, 160)]
            remote(part, part, o_send.at[slot], o_recv.at[slot], partner).wait_send()

    def step(m, _):
        gather = jnp.logical_or(m < 2 * KU - 1, m == 2 * KU - 1 + PRE)

        @pl.when(gather)
        def _():
            gather_step(m - PRE * (m // (2 * KU - 1)))

        @pl.when(jnp.logical_not(gather))
        def _():
            r = m - (2 * KU - 1) - (m >= 2 * KU + PRE).astype(jnp.int32)
            drained(r)
            sum_step(r)

        return 0

    lax.fori_loop(0, 2 * KU + 2 * NU + 5, step, 0)

    for p in range(2):
        remote(sc.at[p], sc.at[p], c_send.at[p], c_recv.at[0], partner).wait_send()
        remote(sb.at[p], sb.at[p], b_send.at[p], b_recv.at[0], partner).wait_send()
        remote(sa.at[p], sa.at[p], a_send.at[p], a_recv.at[0], partner).wait_send()
        pltpu.make_async_copy(yst.at[p], y_ref.at[:, pl.ds(0, NW)], y_sem.at[p]).wait()


def fused(meta, x, wg, wu, wd, sg, su, sd):
    vmem = pl.BlockSpec(memory_space=pltpu.VMEM)
    hbm = pl.BlockSpec(memory_space=pl.ANY)
    dma, regular = pltpu.SemaphoreType.DMA, pltpu.SemaphoreType.REGULAR
    return pl.pallas_call(
        kernel,
        out_shape=jax.ShapeDtypeStruct((256, 2560), BF16),
        in_specs=[vmem, vmem] + [hbm] * 6,
        out_specs=hbm,
        scratch_shapes=[
            pltpu.VMEM((16, 16, 256), F32),
            pltpu.VMEM((8, 160, 256), BF16),
            pltpu.VMEM((8, 256, 384), BF16),
            pltpu.VMEM((HB + 3 * NE, 256, KW), BF16),
            pltpu.VMEM((NE, 2, 256, 1536), F32),
            pltpu.VMEM((NE, 256, KW), BF16),
            pltpu.VMEM((2, 2, KW, 1536), BF16),
            pltpu.VMEM((3, 1536, NW), BF16),
            pltpu.VMEM((NU, 256, NW), F32),
            pltpu.VMEM((RING, 8, 320, NW), BF16),
            pltpu.VMEM((NU, 4, 256, NW), BF16),
            pltpu.VMEM((NU, 2, 256, NW), BF16),
            pltpu.VMEM((NU, 256, NW), BF16),
            pltpu.VMEM((2, 4, 256, NW), BF16),
            pltpu.VMEM((2, 2, 256, NW), BF16),
            pltpu.VMEM((2, 256, NW), BF16),
            pltpu.VMEM((2, 256, NW), BF16),
            dma, dma,
            dma((KU,)), dma((KU,)), dma((KU,)), dma((KU,)), dma((KU,)), dma((KU,)),
            regular((KU,)),
            dma((2, 2)), dma((3,)),
            dma((RING,)), dma((RING,)), regular,
            dma((NU,)), dma((NU,)), dma((NU,)), dma((2,)), dma((2,)), dma((2,)), dma((2,)),
        ],
        compiler_params=pltpu.CompilerParams(
            collective_id=0, has_side_effects=True, vmem_limit_bytes=67043328),
        cost_estimate=pl.CostEstimate(flops=67_000_000_000, bytes_accessed=270_000_000, transcendentals=10_000_000),
        name="moe",
    )(meta, x, wg, wu, wd, sg, su, sd)


def solution(mesh):
    def local(x, expert, slot, gate, wg, wu, wd, sg, su, sd):
        x, expert, slot, gate = x[0, 0], expert[0, 0], slot[0, 0], gate[0, 0]
        code = jnp.where(slot < CAP, expert * CAP + slot, -1).astype(F32)
        weight = gate.astype(BF16).astype(F32)
        meta = jnp.concatenate([code, weight], axis=1).T
        return fused(meta, x, wg, wu, wd, sg, su, sd)[None, None]

    tok = P("dp", "ep", None, None)
    wts = P("ep", None, None)
    return jax.shard_map(
        local, mesh=mesh,
        in_specs=(tok, tok, tok, tok, wts, wts, wts, P(None, None), P(None, None), P(None, None)),
        out_specs=tok, check_vma=False)
```

```python
import functools

import jax
import jax.numpy as jnp
from jax import lax
from jax.experimental import pallas as pl
from jax.experimental.pallas import tpu as pltpu
from jax.sharding import PartitionSpec as P

MESH = pl.DeviceIdType.MESH
F32, BF16 = jnp.float32, jnp.bfloat16
ROWS = ((0, 96), (96, 80), (176, 80))
KU, KW = 5, 512
NU, NW = 10, 256
NE, CAP = 5, 32
RING = 5
LAG = 2, 3, 4
AHEAD = 3
DEEP = 5
HB = 40


def kernel(meta_ref, x_ref, wg_ref, wu_ref, wd_ref, sg_ref, su_ref, sd_ref, y_ref,
           gmeta, onehot, comb, xg, acc, z, wgu, wdn, ys, ob, hb, rc, rb, ra, sc, sb, sa, yst,
           m_send, m_recv, ag_a, ag_b, ag_c, ag_p, ag_s, ag_ps, free,
           gu_sem, dn_sem, x_sem, own_sem, o_recv, o_send, o_free, c_recv, b_recv, a_recv, c_send, b_send, a_send, y_sem):
    me = lax.axis_index("ep")
    core = me % 2
    chip = me // 2
    partner = me + 1 - 2 * core
    dx = 4 * (1 - 2 * ((chip // 4) % 2))
    dy = 2 * (1 - 2 * ((chip // 2) % 2))
    dz = 1 - 2 * (chip % 2)

    def delta(t):
        return dx + t * (dy - dx) + ((t * (t - 1)) // 2) * (dz - 2 * dy + dx)

    def order(i, u):
        return delta((i + u) % 3), delta((i + u + 1) % 3), delta((i + u + 2) % 3)

    def peer(d):
        return 2 * (chip + d) + core

    def remote(src, dst, send, recv, dev):
        return pltpu.make_async_remote_copy(
            src_ref=src, dst_ref=dst, send_sem=send, recv_sem=recv, device_id={"ep": dev}, device_id_type=MESH)

    def start_gu(i):
        slot = i % 3

        for j, (shared_ref, routed_ref) in enumerate(((sg_ref, wg_ref), (su_ref, wu_ref))):
            @pl.when(jnp.logical_and(i < 2 * KU, i % 2 == j))
            def _():
                rows = pl.ds(pl.multiple_of((i // 2) * KW, KW), KW)
                pltpu.make_async_copy(shared_ref.at[rows], wgu.at[slot], gu_sem.at[slot]).start()

            @pl.when(jnp.logical_and(jnp.logical_and(i >= 2 * KU, i < 2 * KU + 4 * KU * NE), i % 2 == j))
            def _():
                m = ((i - 2 * KU) // 2) % (KU * NE)
                rows = pl.ds(pl.multiple_of((m // NE) * KW, KW), KW)
                pltpu.make_async_copy(routed_ref.at[m % NE, rows], wgu.at[slot], gu_sem.at[slot]).start()

    def wait_gu(i):
        slot = i % 3
        pltpu.make_async_copy(sg_ref.at[pl.ds(0, KW)], wgu.at[slot], gu_sem.at[slot]).wait()

    def start_dn(i):
        slot = i % DEEP

        @pl.when(i < NU)
        def _():
            cols = pl.ds(pl.multiple_of(i * NW, NW), NW)
            pltpu.make_async_copy(sd_ref.at[:, cols], wdn.at[slot], dn_sem.at[slot]).start()

        @pl.when(jnp.logical_and(i >= NU, i < NU + NU * NE))
        def _():
            m = i - NU
            cols = pl.ds(pl.multiple_of(((m // NE) % NU) * NW, NW), NW)
            pltpu.make_async_copy(wd_ref.at[m % NE, :, cols], wdn.at[slot], dn_sem.at[slot]).start()

    def wait_dn(i):
        slot = i % DEEP
        pltpu.make_async_copy(sd_ref.at[:, pl.ds(0, NW)], wdn.at[slot], dn_sem.at[slot]).wait()

    def blk(k, s):
        return k * 8 + s

    def own(q):
        k = q % KU
        cols = pl.ds(pl.multiple_of(k * KW, KW), KW)

        @pl.when(q >= KU)
        def _():
            pl.semaphore_wait(free.at[k], 4)

        for stage, sem in enumerate((ag_a, ag_b, ag_c)):
            for i, (r0, rn) in enumerate(ROWS):
                d = order(i, k)[stage]
                remote(x_ref.at[pl.ds(r0, rn), cols], xg.at[blk(k, chip), pl.ds(r0, rn)],
                       ag_s.at[k], sem.at[k], peer(d)).start()
        remote(x_ref.at[:, cols], xg.at[blk(k, chip)], ag_ps.at[k], ag_p.at[k], partner).start()
        pltpu.make_async_copy(x_ref.at[:, cols], xg.at[blk(k, chip)], own_sem.at[k]).start()

    def arrived(sem, k, n):
        remote(xg.at[pl.ds(0, n)], xg.at[pl.ds(0, n)], ag_s.at[k], sem.at[k], partner).wait_recv()

    def forward(b, r0, rn, k, sem, dev):
        part = xg.at[b, pl.ds(r0, rn)]
        remote(part, part, ag_s.at[k], sem.at[k], dev).start()

    def forward_p(b, r0, rn, k):
        part = xg.at[b, pl.ds(r0, rn)]
        remote(part, part, ag_ps.at[k], ag_p.at[k], partner).start()

    def event_a(k):
        arrived(ag_a, k, 1)
        for i, (r0, rn) in enumerate(ROWS):
            a, b, c = order(i, k)
            forward(blk(k, chip + a), r0, rn, k, ag_b, peer(b))
        for i, (r0, rn) in enumerate(ROWS):
            a, b, c = order(i, k)
            forward(blk(k, chip + a), r0, rn, k, ag_c, peer(c))
        for i, (r0, rn) in enumerate(ROWS):
            a, b, c = order(i, k)
            forward_p(blk(k, chip + a), r0, rn, k)

    def event_b(k):
        arrived(ag_b, k, 2)
        for i, (r0, rn) in enumerate(ROWS):
            a, b, c = order(i, k)
            forward(blk(k, chip + b), r0, rn, k, ag_c, peer(c))
            forward(blk(k, chip + b + a), r0, rn, k, ag_c, peer(c))
        for i, (r0, rn) in enumerate(ROWS):
            a, b, c = order(i, k)
            forward_p(blk(k, chip + b), r0, rn, k)
            forward_p(blk(k, chip + b + a), r0, rn, k)

    def event_c(k):
        arrived(ag_c, k, 4)
        for i, (r0, rn) in enumerate(ROWS):
            a, b, c = order(i, k)
            for d in (c, c + a, c + b, c + b + a):
                forward_p(blk(k, chip + d), r0, rn, k)

    def sent(k):
        remote(xg.at[pl.ds(0, 7)], xg.at[pl.ds(0, 7)], ag_s.at[k], ag_a.at[k], partner).wait_send()
        remote(xg.at[pl.ds(0, 8)], xg.at[pl.ds(0, 8)], ag_ps.at[k], ag_p.at[k], partner).wait_send()

    def act(n, store):
        def body(t, _):
            e, r = t // 8, t % 8
            rows = pl.ds(pl.multiple_of(r * 32, 32), 32)
            for q in range(3):
                cols = slice(q * KW, (q + 1) * KW)
                g = acc[e, 0, rows, cols]
                u = acc[e, 1, rows, cols]
                acc[e, 0, rows, cols] = jnp.zeros((32, KW), F32)
                acc[e, 1, rows, cols] = jnp.zeros((32, KW), F32)
                store(e, q, rows, (g * (1.0 / (1.0 + jnp.exp(-g))) * u).astype(BF16))
            return 0

        lax.fori_loop(0, n * 8, body, 0)

    def gate_up(i, lhs, e):
        for j in range(2):
            t = 2 * i + j
            wait_gu(t)
            acc[e, j] += jnp.dot(lhs, wgu[t % 3], preferred_element_type=F32)
            start_gu(t + 3)

    for n in range(NU):
        pltpu.make_async_copy(x_ref.at[:, pl.ds(n * NW, NW)], ob.at[n // 8, n % 8, pl.ds(0, 256)], x_sem.at[n]).start()
    for i in range(3):
        start_gu(jnp.int32(i))
    for i in range(DEEP):
        start_dn(jnp.int32(i))
    barrier = pltpu.get_barrier_semaphore()

    def greet(i, _):
        pl.semaphore_signal(barrier, inc=1, device_id={"ep": (me + i) % 16}, device_id_type=MESH)
        return 0

    lax.fori_loop(1, 16, greet, 0)

    def clear(t, _):
        e, r = t // 8, t % 8
        rows = pl.ds(pl.multiple_of(r * 32, 32), 32)
        for j in range(2):
            acc[e, j, rows] = jnp.zeros((32, 1536), F32)
        return 0

    lax.fori_loop(0, NE * 8, clear, 0)
    pl.semaphore_wait(barrier, 15)

    @pl.when(core == 0)
    def _():
        own(jnp.int32(0))

    def tell(i, _):
        remote(meta_ref, gmeta.at[me], m_send, m_recv, (me + i) % 16).start()
        return 0

    lax.fori_loop(1, 16, tell, 0)
    gmeta[me] = meta_ref[...]

    @pl.when(core == 0)
    def _():
        for k in range(1, AHEAD):
            own(jnp.int32(k))

    def shared(i, _):
        @pl.when(jnp.logical_and(core == 0, i == 1))
        def _():
            event_a(jnp.int32(0))

        @pl.when(jnp.logical_and(core == 0, i == 4))
        def _():
            event_a(jnp.int32(1))

        n = 2 * i
        lhs = jnp.concatenate([ob[n // 8, n % 8, :256], ob[(n + 1) // 8, (n + 1) % 8, :256]], axis=1)
        gate_up(i, lhs, 0)
        return 0

    for n in range(NU):
        pltpu.make_async_copy(x_ref.at[:, pl.ds(n * NW, NW)], ob.at[n // 8, n % 8, pl.ds(0, 256)], x_sem.at[n]).wait()
    lax.fori_loop(0, KU, shared, 0)

    def store_shared(e, q, rows, v):
        for h in range(2):
            n = 2 * q + h
            sc[n // 4, n % 4, rows] = v[:, h * NW:(h + 1) * NW]

    act(1, store_shared)

    def shared_down(i):
        wait_dn(i)
        slot = i % DEEP
        ys[i] = sum(jnp.dot(sc[n // 4, n % 4], wdn[slot, n * NW:(n + 1) * NW], preferred_element_type=F32)
                    for n in range(6))
        start_dn(i + DEEP)

    def build_comb(s):
        m = gmeta[2 * s + core]
        row = lax.broadcasted_iota(jnp.int32, (384, 256), 0)
        mine = (me * (NE * CAP)).astype(jnp.int32)
        theirs = (partner * (NE * CAP)).astype(jnp.int32)
        target = jnp.where(row < 160, row + mine, jnp.where(row < 320, row - 160 + theirs, -7)).astype(F32)
        t = jnp.zeros((384, 256), F32)
        for j in range(8):
            t = t + jnp.where(target == m[j:j + 1], m[8 + j:9 + j], 0.0)
        comb[s] = t.T.astype(BF16)

    @pl.when(core == 0)
    def _():
        event_b(jnp.int32(0))

    remote(gmeta.at[pl.ds(0, 15)], gmeta.at[pl.ds(0, 15)], m_send, m_recv, partner).wait()

    def gather_step(g):
        ph, k = g // KU, g % KU
        nxt = g + 1

        @pl.when(core == ph)
        def _():
            event_c(k)
            pltpu.make_async_copy(x_ref.at[:, pl.ds(0, KW)], xg.at[blk(k, chip)], own_sem.at[k]).wait()

        @pl.when(core != ph)
        def _():
            arrived(ag_p, k, 8)

        @pl.when(jnp.logical_and(nxt < 2 * KU, core == nxt // KU))
        def _():
            event_b(nxt % KU)

        @pl.when(jnp.logical_and(g + 2 < 2 * KU, core == (g + 2) // KU))
        def _():
            event_a((g + 2) % KU)

        @pl.when(jnp.logical_and(g + AHEAD < KU, core == 0))
        def _():
            own(g + AHEAD)

        @pl.when(k == 0)
        def _():
            def build(s, _):
                m = gmeta[2 * s + ph]
                target = (lax.broadcasted_iota(jnp.int32, (160, 256), 0) + me * (NE * CAP)).astype(F32)
                t = jnp.zeros((160, 256), F32)
                for j in range(8):
                    t = jnp.where(target == m[j:j + 1], 1.0, t)
                onehot[s] = t.astype(BF16)
                return 0

            lax.fori_loop(0, 8, build, 0)

        for s in range(8):
            zs = jnp.dot(onehot[s], xg[blk(k, s)], preferred_element_type=F32).astype(BF16)
            for e in range(NE):
                z[e, s * CAP:(s + 1) * CAP] = zs[e * CAP:(e + 1) * CAP]

        def expert(e, _):
            @pl.when(e == 2)
            def _():
                @pl.when(jnp.logical_and(jnp.logical_and(g >= 2, g <= 6), core == 1))
                def _():
                    own(g + 3)

            gate_up(KU + g * NE + e, z[e], e)
            return 0

        lax.fori_loop(0, NE, expert, 0)

        @pl.when(g < NU // 2)
        def _():
            shared_down(2 * g)
            shared_down(2 * g + 1)

        @pl.when(g < 4)
        def _():
            build_comb(2 * g)
            build_comb(2 * g + 1)

        @pl.when(jnp.logical_and(ph == 0, core == 0))
        def _():
            sent(k)
            pl.semaphore_signal(free.at[k], inc=1, device_id={"ep": partner}, device_id_type=MESH)

        @pl.when(jnp.logical_and(ph == 0, core == 1))
        def _():
            for d in (dx, dy, dz):
                pl.semaphore_signal(free.at[k], inc=1, device_id={"ep": peer(d)}, device_id_type=MESH)

        @pl.when(k == KU - 1)
        def _():
            @pl.when(jnp.logical_and(ph == 1, core == 1))
            def _():
                for kk in range(KU):
                    sent(kk)

            def store(e, q, rows, v):
                xg[HB * (1 - ph) + e * 3 + q, rows] = v

            act(NE, store)

    def term(slot, d, r0, rn):
        return jnp.dot(comb[d, r0:r0 + rn, :320], ob[slot, d], preferred_element_type=F32)

    def sum_step(r):
        def main(v):
            return jnp.logical_and(v >= 0, v < NU)

        v4 = r - LAG[2]

        @pl.when(main(v4))
        def _():
            u, slot, p = v4, v4 % RING, v4 % 2
            remote(ra.at[u], ra.at[u], a_send.at[0], a_recv.at[u], partner).wait_recv()
            val = term(slot, chip, 0, 256) + rc[u, 0].astype(F32) + rb[u, 0].astype(F32) + ra[u].astype(F32) + ys[u]

            @pl.when(u >= 2)
            def _():
                pltpu.make_async_copy(yst.at[p], y_ref.at[:, pl.ds(0, NW)], y_sem.at[p]).wait()

            yst[p] = val.astype(BF16)
            cols = pl.ds(pl.multiple_of(u * NW, NW), NW)
            pltpu.make_async_copy(yst.at[p], y_ref.at[:, cols], y_sem.at[p]).start()

            @pl.when(u < NU - RING)
            def _():
                pl.semaphore_signal(o_free, inc=1, device_id={"ep": partner}, device_id_type=MESH)

        v3 = r - LAG[1]

        @pl.when(main(v3))
        def _():
            u, slot, p = v3, v3 % RING, v3 % 2
            remote(rb.at[u], rb.at[u], b_send.at[0], b_recv.at[u], partner).wait_recv()

            @pl.when(u >= 2)
            def _():
                remote(sa.at[p], sa.at[p], a_send.at[p], a_recv.at[0], partner).wait_send()

            for i, (r0, rn) in enumerate(ROWS):
                a, b, c = order(i, u)
                rows = slice(r0, r0 + rn)
                val = term(slot, chip + a, r0, rn) + rc[u, 1, rows].astype(F32) + rb[u, 1, rows].astype(F32)
                sa[p, rows] = val.astype(BF16)
            for i, (r0, rn) in enumerate(ROWS):
                a, b, c = order(i, u)
                remote(sa.at[p, pl.ds(r0, rn)], ra.at[u, pl.ds(r0, rn)], a_send.at[p], a_recv.at[u], peer(a)).start()

        v2 = r - LAG[0]

        @pl.when(main(v2))
        def _():
            u, slot, p = v2, v2 % RING, v2 % 2
            remote(rc.at[u], rc.at[u], c_send.at[0], c_recv.at[u], partner).wait_recv()

            @pl.when(u >= 2)
            def _():
                remote(sb.at[p], sb.at[p], b_send.at[p], b_recv.at[0], partner).wait_send()

            for i, (r0, rn) in enumerate(ROWS):
                a, b, c = order(i, u)
                rows = slice(r0, r0 + rn)
                for h in range(2):
                    val = term(slot, chip + b + h * a, r0, rn) + rc[u, 2 + h, rows].astype(F32)
                    sb[p, h, rows] = val.astype(BF16)
            for i, (r0, rn) in enumerate(ROWS):
                a, b, c = order(i, u)
                remote(sb.at[p, :, pl.ds(r0, rn)], rb.at[u, :, pl.ds(r0, rn)], b_send.at[p], b_recv.at[u],
                       peer(b)).start()

        @pl.when(r < NU)
        def _():
            slot, p = r % RING, r % 2
            there = hb.at[p], ob.at[slot, :, pl.ds(160, 160)], o_send.at[p], o_recv.at[slot], partner

            @pl.when(r >= 2)
            def _():
                remote(*there).wait_send()

            for e in range(NE):
                i = NU + r * NE + e
                wait_dn(i)
                own_o, other_o = (
                    sum(jnp.dot(xg[base + e * 3 + q], wdn[i % DEEP, q * KW:(q + 1) * KW],
                                preferred_element_type=F32) for q in range(3)).astype(BF16)
                    for base in (HB * (1 - core), HB * core))
                for s in range(8):
                    ob[slot, s, e * CAP:(e + 1) * CAP] = own_o[s * CAP:(s + 1) * CAP]
                    hb[p, s, e * CAP:(e + 1) * CAP] = other_o[s * CAP:(s + 1) * CAP]
                start_dn(i + DEEP)

            @pl.when(r >= RING)
            def _():
                pl.semaphore_wait(o_free, 1)

            remote(*there).start()

        v1 = r

        @pl.when(main(v1))
        def _():
            u, slot, p = v1, v1 % RING, v1 % 3
            part = ob.at[slot, :, pl.ds(160, 160)]
            remote(part, part, o_send.at[slot], o_recv.at[slot], partner).wait_recv()

            @pl.when(u >= 3)
            def _():
                remote(sc.at[p], sc.at[p], c_send.at[p], c_recv.at[0], partner).wait_send()

            for i, (r0, rn) in enumerate(ROWS):
                a, b, c = order(i, u)
                rows = slice(r0, r0 + rn)
                for h in range(4):
                    val = term(slot, chip + c + (h // 2) * b + (h % 2) * a, r0, rn)
                    sc[p, h, rows] = val.astype(BF16)
            for i, (r0, rn) in enumerate(ROWS):
                a, b, c = order(i, u)
                remote(sc.at[p, :, pl.ds(r0, rn)], rc.at[u, :, pl.ds(r0, rn)], c_send.at[p], c_recv.at[u],
                       peer(c)).start()

    def step(m, _):
        @pl.when(m < 2 * KU)
        def _():
            gather_step(m)

        @pl.when(m >= 2 * KU)
        def _():
            sum_step(m - 2 * KU)

        return 0

    lax.fori_loop(0, 2 * KU + NU + LAG[2], step, 0)

    for p in range(3):
        remote(sc.at[p], sc.at[p], c_send.at[p], c_recv.at[0], partner).wait_send()
    for p in range(2):
        part = ob.at[0, :, pl.ds(160, 160)]
        remote(hb.at[p], part, o_send.at[p], o_recv.at[0], partner).wait_send()
        remote(sb.at[p], sb.at[p], b_send.at[p], b_recv.at[0], partner).wait_send()
        remote(sa.at[p], sa.at[p], a_send.at[p], a_recv.at[0], partner).wait_send()
        pltpu.make_async_copy(yst.at[p], y_ref.at[:, pl.ds(0, NW)], y_sem.at[p]).wait()


def fused(meta, x, wg, wu, wd, sg, su, sd):
    vmem = pl.BlockSpec(memory_space=pltpu.VMEM)
    hbm = pl.BlockSpec(memory_space=pl.ANY)
    dma, regular = pltpu.SemaphoreType.DMA, pltpu.SemaphoreType.REGULAR
    return pl.pallas_call(
        kernel,
        out_shape=jax.ShapeDtypeStruct((256, 2560), BF16),
        in_specs=[vmem] + [hbm] * 7,
        out_specs=hbm,
        scratch_shapes=[
            pltpu.VMEM((16, 16, 256), F32),
            pltpu.VMEM((8, 160, 256), BF16),
            pltpu.VMEM((8, 256, 384), BF16),
            pltpu.VMEM((HB + 3 * NE, 256, KW), BF16),
            pltpu.VMEM((NE, 2, 256, 1536), F32),
            pltpu.VMEM((NE, 256, KW), BF16),
            pltpu.VMEM((3, KW, 1536), BF16),
            pltpu.VMEM((DEEP, 1536, NW), BF16),
            pltpu.VMEM((NU, 256, NW), F32),
            pltpu.VMEM((RING, 8, 320, NW), BF16),
            pltpu.VMEM((2, 8, 160, NW), BF16),
            pltpu.VMEM((NU, 4, 256, NW), BF16),
            pltpu.VMEM((NU, 2, 256, NW), BF16),
            pltpu.VMEM((NU, 256, NW), BF16),
            pltpu.VMEM((3, 4, 256, NW), BF16),
            pltpu.VMEM((2, 2, 256, NW), BF16),
            pltpu.VMEM((2, 256, NW), BF16),
            pltpu.VMEM((2, 256, NW), BF16),
            dma, dma,
            dma((KU,)), dma((KU,)), dma((KU,)), dma((KU,)), dma((KU,)), dma((KU,)),
            regular((KU,)),
            dma((3,)), dma((DEEP,)), dma((NU,)), dma((KU,)),
            dma((RING,)), dma((2,)), regular,
            dma((NU,)), dma((NU,)), dma((NU,)), dma((3,)), dma((2,)), dma((2,)), dma((2,)),
        ],
        compiler_params=pltpu.CompilerParams(
            collective_id=0, has_side_effects=True, vmem_limit_bytes=67043328),
        cost_estimate=pl.CostEstimate(flops=67_000_000_000, bytes_accessed=270_000_000, transcendentals=10_000_000),
        name="moe",
    )(meta, x, wg, wu, wd, sg, su, sd)


def solution(mesh):
    def local(x, expert, slot, gate, wg, wu, wd, sg, su, sd):
        x, expert, slot, gate = x[0, 0], expert[0, 0], slot[0, 0], gate[0, 0]
        code = jnp.where(slot < CAP, expert * CAP + slot, -1).astype(F32)
        weight = gate.astype(BF16).astype(F32)
        meta = jnp.concatenate([code, weight], axis=1).T
        return fused(meta, x, wg, wu, wd, sg, su, sd)[None, None]

    tok = P("dp", "ep", None, None)
    wts = P("ep", None, None)
    return jax.shard_map(
        local, mesh=mesh,
        in_specs=(tok, tok, tok, tok, wts, wts, wts, P(None, None), P(None, None), P(None, None)),
        out_specs=tok, check_vma=False)
```

```python
import functools

import jax
import jax.numpy as jnp
from jax import lax
from jax.experimental import pallas as pl
from jax.experimental.pallas import tpu as pltpu
from jax.sharding import PartitionSpec as P

MESH = pl.DeviceIdType.MESH
F32, BF16 = jnp.float32, jnp.bfloat16
ROWS = ((0, 96), (96, 80), (176, 80))
KU, KW = 5, 512
NU, NW = 10, 256
NE, CAP = 5, 32
RING = 5
LAG = 3, 4, 5
AHEAD = 3
DEEP = 5
HB = 40


def kernel(meta_ref, x_ref, wg_ref, wu_ref, wd_ref, sg_ref, su_ref, sd_ref, y_ref,
           gmeta, onehot, comb, xg, acc, z, wgu, wdn, ys, ob, hb, rc, rb, ra, sc, sb, sa, yst,
           m_send, m_recv, ag_a, ag_b, ag_c, ag_p, ag_s, ag_ps, free,
           gu_sem, dn_sem, x_sem, own_sem, o_recv, o_send, o_free, c_recv, b_recv, a_recv, c_send, b_send, a_send, y_sem):
    me = lax.axis_index("ep")
    core = me % 2
    chip = me // 2
    partner = me + 1 - 2 * core
    dx = 4 * (1 - 2 * ((chip // 4) % 2))
    dy = 2 * (1 - 2 * ((chip // 2) % 2))
    dz = 1 - 2 * (chip % 2)

    def delta(t):
        return dx + t * (dy - dx) + ((t * (t - 1)) // 2) * (dz - 2 * dy + dx)

    def order(i, u):
        return delta((i + u) % 3), delta((i + u + 1) % 3), delta((i + u + 2) % 3)

    def peer(d):
        return 2 * (chip + d) + core

    def remote(src, dst, send, recv, dev):
        return pltpu.make_async_remote_copy(
            src_ref=src, dst_ref=dst, send_sem=send, recv_sem=recv, device_id={"ep": dev}, device_id_type=MESH)

    def start_gu(i):
        slot = i % 3

        for j, (shared_ref, routed_ref) in enumerate(((sg_ref, wg_ref), (su_ref, wu_ref))):
            @pl.when(jnp.logical_and(i < 2 * KU, i % 2 == j))
            def _():
                rows = pl.ds(pl.multiple_of((i // 2) * KW, KW), KW)
                pltpu.make_async_copy(shared_ref.at[rows], wgu.at[slot], gu_sem.at[slot]).start()

            @pl.when(jnp.logical_and(jnp.logical_and(i >= 2 * KU, i < 2 * KU + 4 * KU * NE), i % 2 == j))
            def _():
                m = ((i - 2 * KU) // 2) % (KU * NE)
                rows = pl.ds(pl.multiple_of((m // NE) * KW, KW), KW)
                pltpu.make_async_copy(routed_ref.at[m % NE, rows], wgu.at[slot], gu_sem.at[slot]).start()

    def wait_gu(i):
        slot = i % 3
        pltpu.make_async_copy(sg_ref.at[pl.ds(0, KW)], wgu.at[slot], gu_sem.at[slot]).wait()

    def start_dn(i):
        slot = i % DEEP

        @pl.when(i < NU)
        def _():
            cols = pl.ds(pl.multiple_of(i * NW, NW), NW)
            pltpu.make_async_copy(sd_ref.at[:, cols], wdn.at[slot], dn_sem.at[slot]).start()

        @pl.when(jnp.logical_and(i >= NU, i < NU + NU * NE))
        def _():
            m = i - NU
            cols = pl.ds(pl.multiple_of(((m // NE) % NU) * NW, NW), NW)
            pltpu.make_async_copy(wd_ref.at[m % NE, :, cols], wdn.at[slot], dn_sem.at[slot]).start()

    def wait_dn(i):
        slot = i % DEEP
        pltpu.make_async_copy(sd_ref.at[:, pl.ds(0, NW)], wdn.at[slot], dn_sem.at[slot]).wait()

    def blk(k, s):
        return k * 8 + s

    def own(q):
        k = q % KU
        cols = pl.ds(pl.multiple_of(k * KW, KW), KW)

        @pl.when(q >= KU)
        def _():
            pl.semaphore_wait(free.at[k], 4)

        for stage, sem in enumerate((ag_a, ag_b, ag_c)):
            for i, (r0, rn) in enumerate(ROWS):
                d = order(i, k)[stage]
                remote(x_ref.at[pl.ds(r0, rn), cols], xg.at[blk(k, chip), pl.ds(r0, rn)],
                       ag_s.at[k], sem.at[k], peer(d)).start()
        remote(x_ref.at[:, cols], xg.at[blk(k, chip)], ag_ps.at[k], ag_p.at[k], partner).start()
        pltpu.make_async_copy(x_ref.at[:, cols], xg.at[blk(k, chip)], own_sem.at[k]).start()

    def arrived(sem, k, n):
        remote(xg.at[pl.ds(0, n)], xg.at[pl.ds(0, n)], ag_s.at[k], sem.at[k], partner).wait_recv()

    def forward(b, r0, rn, k, sem, dev):
        part = xg.at[b, pl.ds(r0, rn)]
        remote(part, part, ag_s.at[k], sem.at[k], dev).start()

    def forward_p(b, r0, rn, k):
        part = xg.at[b, pl.ds(r0, rn)]
        remote(part, part, ag_ps.at[k], ag_p.at[k], partner).start()

    def event_a(k):
        arrived(ag_a, k, 1)
        for i, (r0, rn) in enumerate(ROWS):
            a, b, c = order(i, k)
            forward(blk(k, chip + a), r0, rn, k, ag_b, peer(b))
        for i, (r0, rn) in enumerate(ROWS):
            a, b, c = order(i, k)
            forward(blk(k, chip + a), r0, rn, k, ag_c, peer(c))
        for i, (r0, rn) in enumerate(ROWS):
            a, b, c = order(i, k)
            forward_p(blk(k, chip + a), r0, rn, k)

    def event_b(k):
        arrived(ag_b, k, 2)
        for i, (r0, rn) in enumerate(ROWS):
            a, b, c = order(i, k)
            forward(blk(k, chip + b), r0, rn, k, ag_c, peer(c))
            forward(blk(k, chip + b + a), r0, rn, k, ag_c, peer(c))
        for i, (r0, rn) in enumerate(ROWS):
            a, b, c = order(i, k)
            forward_p(blk(k, chip + b), r0, rn, k)
            forward_p(blk(k, chip + b + a), r0, rn, k)

    def event_c(k):
        arrived(ag_c, k, 4)
        for i, (r0, rn) in enumerate(ROWS):
            a, b, c = order(i, k)
            for d in (c, c + a, c + b, c + b + a):
                forward_p(blk(k, chip + d), r0, rn, k)

    def sent(k):
        remote(xg.at[pl.ds(0, 7)], xg.at[pl.ds(0, 7)], ag_s.at[k], ag_a.at[k], partner).wait_send()
        remote(xg.at[pl.ds(0, 8)], xg.at[pl.ds(0, 8)], ag_ps.at[k], ag_p.at[k], partner).wait_send()

    def act(n, store):
        def body(t, _):
            e, r = t // 8, t % 8
            rows = pl.ds(pl.multiple_of(r * 32, 32), 32)
            for q in range(3):
                cols = slice(q * KW, (q + 1) * KW)
                g = acc[e, 0, rows, cols]
                u = acc[e, 1, rows, cols]
                acc[e, 0, rows, cols] = jnp.zeros((32, KW), F32)
                acc[e, 1, rows, cols] = jnp.zeros((32, KW), F32)
                store(e, q, rows, (g * (1.0 / (1.0 + jnp.exp(-g))) * u).astype(BF16))
            return 0

        lax.fori_loop(0, n * 8, body, 0)

    def gate_up(i, lhs, e):
        for j in range(2):
            t = 2 * i + j
            wait_gu(t)
            acc[e, j] += jnp.dot(lhs, wgu[t % 3], preferred_element_type=F32)
            start_gu(t + 3)

    for n in range(NU):
        pltpu.make_async_copy(x_ref.at[:, pl.ds(n * NW, NW)], ob.at[n // 8, n % 8, pl.ds(0, 256)], x_sem.at[n]).start()
    for i in range(3):
        start_gu(jnp.int32(i))
    for i in range(DEEP):
        start_dn(jnp.int32(i))
    barrier = pltpu.get_barrier_semaphore()

    def greet(i, _):
        pl.semaphore_signal(barrier, inc=1, device_id={"ep": (me + i) % 16}, device_id_type=MESH)
        return 0

    lax.fori_loop(1, 16, greet, 0)

    def clear(t, _):
        e, r = t // 8, t % 8
        rows = pl.ds(pl.multiple_of(r * 32, 32), 32)
        for j in range(2):
            acc[e, j, rows] = jnp.zeros((32, 1536), F32)
        return 0

    lax.fori_loop(0, NE * 8, clear, 0)
    pl.semaphore_wait(barrier, 15)

    @pl.when(core == 0)
    def _():
        own(jnp.int32(0))

    def tell(i, _):
        remote(meta_ref, gmeta.at[me], m_send, m_recv, (me + i) % 16).start()
        return 0

    lax.fori_loop(1, 16, tell, 0)
    gmeta[me] = meta_ref[...]

    @pl.when(core == 0)
    def _():
        for k in range(1, AHEAD):
            own(jnp.int32(k))

    def shared(i, _):
        @pl.when(jnp.logical_and(core == 0, i == 1))
        def _():
            event_a(jnp.int32(0))

        @pl.when(jnp.logical_and(core == 0, i == 4))
        def _():
            event_a(jnp.int32(1))

        n = 2 * i
        lhs = jnp.concatenate([ob[n // 8, n % 8, :256], ob[(n + 1) // 8, (n + 1) % 8, :256]], axis=1)
        gate_up(i, lhs, 0)
        return 0

    for n in range(NU):
        pltpu.make_async_copy(x_ref.at[:, pl.ds(n * NW, NW)], ob.at[n // 8, n % 8, pl.ds(0, 256)], x_sem.at[n]).wait()
    lax.fori_loop(0, KU, shared, 0)

    def store_shared(e, q, rows, v):
        for h in range(2):
            n = 2 * q + h
            sc[n // 4, n % 4, rows] = v[:, h * NW:(h + 1) * NW]

    act(1, store_shared)

    def shared_down(i):
        wait_dn(i)
        slot = i % DEEP
        ys[i] = sum(jnp.dot(sc[n // 4, n % 4], wdn[slot, n * NW:(n + 1) * NW], preferred_element_type=F32)
                    for n in range(6))
        start_dn(i + DEEP)

    def build_comb(s):
        m = gmeta[2 * s + core]
        row = lax.broadcasted_iota(jnp.int32, (384, 256), 0)
        mine = (me * (NE * CAP)).astype(jnp.int32)
        theirs = (partner * (NE * CAP)).astype(jnp.int32)
        target = jnp.where(row < 160, row + mine, jnp.where(row < 320, row - 160 + theirs, -7)).astype(F32)
        t = jnp.zeros((384, 256), F32)
        for j in range(8):
            t = t + jnp.where(target == m[j:j + 1], m[8 + j:9 + j], 0.0)
        comb[s] = t.T.astype(BF16)

    @pl.when(core == 0)
    def _():
        event_b(jnp.int32(0))

    remote(gmeta.at[pl.ds(0, 15)], gmeta.at[pl.ds(0, 15)], m_send, m_recv, partner).wait()

    def gather_step(g):
        ph, k = g // KU, g % KU
        nxt = g + 1

        @pl.when(core == ph)
        def _():
            event_c(k)
            pltpu.make_async_copy(x_ref.at[:, pl.ds(0, KW)], xg.at[blk(k, chip)], own_sem.at[k]).wait()

        @pl.when(core != ph)
        def _():
            arrived(ag_p, k, 8)

        @pl.when(jnp.logical_and(nxt < 2 * KU, core == nxt // KU))
        def _():
            event_b(nxt % KU)

        @pl.when(jnp.logical_and(g + 2 < 2 * KU, core == (g + 2) // KU))
        def _():
            event_a((g + 2) % KU)

        @pl.when(jnp.logical_and(g + AHEAD < KU, core == 0))
        def _():
            own(g + AHEAD)

        @pl.when(k == 0)
        def _():
            def build(s, _):
                m = gmeta[2 * s + ph]
                target = (lax.broadcasted_iota(jnp.int32, (160, 256), 0) + me * (NE * CAP)).astype(F32)
                t = jnp.zeros((160, 256), F32)
                for j in range(8):
                    t = jnp.where(target == m[j:j + 1], 1.0, t)
                onehot[s] = t.astype(BF16)
                return 0

            lax.fori_loop(0, 8, build, 0)

        for s in range(8):
            zs = jnp.dot(onehot[s], xg[blk(k, s)], preferred_element_type=F32).astype(BF16)
            for e in range(NE):
                z[e, s * CAP:(s + 1) * CAP] = zs[e * CAP:(e + 1) * CAP]

        def expert(e, _):
            @pl.when(e == 2)
            def _():
                @pl.when(jnp.logical_and(jnp.logical_and(g >= 2, g <= 6), core == 1))
                def _():
                    own(g + 3)

            gate_up(KU + g * NE + e, z[e], e)
            return 0

        lax.fori_loop(0, NE, expert, 0)

        @pl.when(g < NU // 2)
        def _():
            shared_down(2 * g)
            shared_down(2 * g + 1)

        @pl.when(g < 4)
        def _():
            build_comb(2 * g)
            build_comb(2 * g + 1)

        @pl.when(jnp.logical_and(ph == 0, core == 0))
        def _():
            sent(k)
            pl.semaphore_signal(free.at[k], inc=1, device_id={"ep": partner}, device_id_type=MESH)

        @pl.when(jnp.logical_and(ph == 0, core == 1))
        def _():
            for d in (dx, dy, dz):
                pl.semaphore_signal(free.at[k], inc=1, device_id={"ep": peer(d)}, device_id_type=MESH)

        @pl.when(k == KU - 1)
        def _():
            @pl.when(jnp.logical_and(ph == 1, core == 1))
            def _():
                for kk in range(KU):
                    sent(kk)

            def store(e, q, rows, v):
                xg[HB * (1 - ph) + e * 3 + q, rows] = v

            act(NE, store)

    def term(slot, d, r0, rn):
        return jnp.dot(comb[d, r0:r0 + rn, :320], ob[slot, d], preferred_element_type=F32)

    def sum_step(r):
        def main(v):
            return jnp.logical_and(v >= 0, v < NU)

        v4 = r - LAG[2]

        @pl.when(main(v4))
        def _():
            u, slot, p = v4, v4 % RING, v4 % 2
            remote(ra.at[u], ra.at[u], a_send.at[0], a_recv.at[u], partner).wait_recv()
            val = term(slot, chip, 0, 256) + rc[u, 0].astype(F32) + rb[u, 0].astype(F32) + ra[u].astype(F32) + ys[u]

            @pl.when(u >= 2)
            def _():
                pltpu.make_async_copy(yst.at[p], y_ref.at[:, pl.ds(0, NW)], y_sem.at[p]).wait()

            yst[p] = val.astype(BF16)
            cols = pl.ds(pl.multiple_of(u * NW, NW), NW)
            pltpu.make_async_copy(yst.at[p], y_ref.at[:, cols], y_sem.at[p]).start()

            @pl.when(u < NU - RING)
            def _():
                pl.semaphore_signal(o_free, inc=1, device_id={"ep": partner}, device_id_type=MESH)

        v3 = r - LAG[1]

        @pl.when(main(v3))
        def _():
            u, slot, p = v3, v3 % RING, v3 % 2
            remote(rb.at[u], rb.at[u], b_send.at[0], b_recv.at[u], partner).wait_recv()

            @pl.when(u >= 2)
            def _():
                remote(sa.at[p], sa.at[p], a_send.at[p], a_recv.at[0], partner).wait_send()

            for i, (r0, rn) in enumerate(ROWS):
                a, b, c = order(i, u)
                rows = slice(r0, r0 + rn)
                val = term(slot, chip + a, r0, rn) + rc[u, 1, rows].astype(F32) + rb[u, 1, rows].astype(F32)
                sa[p, rows] = val.astype(BF16)
            for i, (r0, rn) in enumerate(ROWS):
                a, b, c = order(i, u)
                remote(sa.at[p, pl.ds(r0, rn)], ra.at[u, pl.ds(r0, rn)], a_send.at[p], a_recv.at[u], peer(a)).start()

        v2 = r - LAG[0]

        @pl.when(main(v2))
        def _():
            u, slot, p = v2, v2 % RING, v2 % 2
            remote(rc.at[u], rc.at[u], c_send.at[0], c_recv.at[u], partner).wait_recv()

            @pl.when(u >= 2)
            def _():
                remote(sb.at[p], sb.at[p], b_send.at[p], b_recv.at[0], partner).wait_send()

            for i, (r0, rn) in enumerate(ROWS):
                a, b, c = order(i, u)
                rows = slice(r0, r0 + rn)
                for h in range(2):
                    val = term(slot, chip + b + h * a, r0, rn) + rc[u, 2 + h, rows].astype(F32)
                    sb[p, h, rows] = val.astype(BF16)
            for i, (r0, rn) in enumerate(ROWS):
                a, b, c = order(i, u)
                remote(sb.at[p, :, pl.ds(r0, rn)], rb.at[u, :, pl.ds(r0, rn)], b_send.at[p], b_recv.at[u],
                       peer(b)).start()

        @pl.when(r < NU)
        def _():
            slot, p = r % RING, r % 2
            there = hb.at[p], ob.at[slot, :, pl.ds(160, 160)], o_send.at[p], o_recv.at[slot], partner

            @pl.when(r >= 2)
            def _():
                remote(*there).wait_send()

            for e in range(NE):
                i = NU + r * NE + e
                wait_dn(i)
                own_o, other_o = (
                    sum(jnp.dot(xg[base + e * 3 + q], wdn[i % DEEP, q * KW:(q + 1) * KW],
                                preferred_element_type=F32) for q in range(3)).astype(BF16)
                    for base in (HB * (1 - core), HB * core))
                for s in range(8):
                    ob[slot, s, e * CAP:(e + 1) * CAP] = own_o[s * CAP:(s + 1) * CAP]
                    hb[p, s, e * CAP:(e + 1) * CAP] = other_o[s * CAP:(s + 1) * CAP]
                start_dn(i + DEEP)

            @pl.when(r >= RING)
            def _():
                pl.semaphore_wait(o_free, 1)

            remote(*there).start()

        v1 = r - 1

        @pl.when(main(v1))
        def _():
            u, slot, p = v1, v1 % RING, v1 % 3
            part = ob.at[slot, :, pl.ds(160, 160)]
            remote(part, part, o_send.at[slot], o_recv.at[slot], partner).wait_recv()

            @pl.when(u >= 3)
            def _():
                remote(sc.at[p], sc.at[p], c_send.at[p], c_recv.at[0], partner).wait_send()

            for i, (r0, rn) in enumerate(ROWS):
                a, b, c = order(i, u)
                rows = slice(r0, r0 + rn)
                for h in range(4):
                    val = term(slot, chip + c + (h // 2) * b + (h % 2) * a, r0, rn)
                    sc[p, h, rows] = val.astype(BF16)
            for i, (r0, rn) in enumerate(ROWS):
                a, b, c = order(i, u)
                remote(sc.at[p, :, pl.ds(r0, rn)], rc.at[u, :, pl.ds(r0, rn)], c_send.at[p], c_recv.at[u],
                       peer(c)).start()

    def step(m, _):
        @pl.when(m < 2 * KU)
        def _():
            gather_step(m)

        @pl.when(m >= 2 * KU)
        def _():
            sum_step(m - 2 * KU)

        return 0

    lax.fori_loop(0, 2 * KU + NU + LAG[2], step, 0)

    for p in range(3):
        remote(sc.at[p], sc.at[p], c_send.at[p], c_recv.at[0], partner).wait_send()
    for p in range(2):
        part = ob.at[0, :, pl.ds(160, 160)]
        remote(hb.at[p], part, o_send.at[p], o_recv.at[0], partner).wait_send()
        remote(sb.at[p], sb.at[p], b_send.at[p], b_recv.at[0], partner).wait_send()
        remote(sa.at[p], sa.at[p], a_send.at[p], a_recv.at[0], partner).wait_send()
        pltpu.make_async_copy(yst.at[p], y_ref.at[:, pl.ds(0, NW)], y_sem.at[p]).wait()


def fused(meta, x, wg, wu, wd, sg, su, sd):
    vmem = pl.BlockSpec(memory_space=pltpu.VMEM)
    hbm = pl.BlockSpec(memory_space=pl.ANY)
    dma, regular = pltpu.SemaphoreType.DMA, pltpu.SemaphoreType.REGULAR
    return pl.pallas_call(
        kernel,
        out_shape=jax.ShapeDtypeStruct((256, 2560), BF16),
        in_specs=[vmem] + [hbm] * 7,
        out_specs=hbm,
        scratch_shapes=[
            pltpu.VMEM((16, 16, 256), F32),
            pltpu.VMEM((8, 160, 256), BF16),
            pltpu.VMEM((8, 256, 384), BF16),
            pltpu.VMEM((HB + 3 * NE, 256, KW), BF16),
            pltpu.VMEM((NE, 2, 256, 1536), F32),
            pltpu.VMEM((NE, 256, KW), BF16),
            pltpu.VMEM((3, KW, 1536), BF16),
            pltpu.VMEM((DEEP, 1536, NW), BF16),
            pltpu.VMEM((NU, 256, NW), F32),
            pltpu.VMEM((RING, 8, 320, NW), BF16),
            pltpu.VMEM((2, 8, 160, NW), BF16),
            pltpu.VMEM((NU, 4, 256, NW), BF16),
            pltpu.VMEM((NU, 2, 256, NW), BF16),
            pltpu.VMEM((NU, 256, NW), BF16),
            pltpu.VMEM((3, 4, 256, NW), BF16),
            pltpu.VMEM((2, 2, 256, NW), BF16),
            pltpu.VMEM((2, 256, NW), BF16),
            pltpu.VMEM((2, 256, NW), BF16),
            dma, dma,
            dma((KU,)), dma((KU,)), dma((KU,)), dma((KU,)), dma((KU,)), dma((KU,)),
            regular((KU,)),
            dma((3,)), dma((DEEP,)), dma((NU,)), dma((KU,)),
            dma((RING,)), dma((2,)), regular,
            dma((NU,)), dma((NU,)), dma((NU,)), dma((3,)), dma((2,)), dma((2,)), dma((2,)),
        ],
        compiler_params=pltpu.CompilerParams(
            collective_id=0, has_side_effects=True, vmem_limit_bytes=67043328),
        cost_estimate=pl.CostEstimate(flops=67_000_000_000, bytes_accessed=270_000_000, transcendentals=10_000_000),
        name="moe",
    )(meta, x, wg, wu, wd, sg, su, sd)


def solution(mesh):
    def local(x, expert, slot, gate, wg, wu, wd, sg, su, sd):
        x, expert, slot, gate = x[0, 0], expert[0, 0], slot[0, 0], gate[0, 0]
        code = jnp.where(slot < CAP, expert * CAP + slot, -1).astype(F32)
        weight = gate.astype(BF16).astype(F32)
        meta = jnp.concatenate([code, weight], axis=1).T
        return fused(meta, x, wg, wu, wd, sg, su, sd)[None, None]

    tok = P("dp", "ep", None, None)
    wts = P("ep", None, None)
    return jax.shard_map(
        local, mesh=mesh,
        in_specs=(tok, tok, tok, tok, wts, wts, wts, P(None, None), P(None, None), P(None, None)),
        out_specs=tok, check_vma=False)
```
